256 devices in a mesh: dp: 8 (over y, core), expert: 8 (over z), tile: 4 (over x).
Axes of the slice: x: 4, y: 4, z: 8, core: 2. Of those that a mesh axis runs over, the one named last changes fastest.
Arguments:
- tokens: bfloat16 [4096, 4096], P(('dp', 'expert'), 'tile'), may hold values from -6 to 6
- hidden: bfloat16 [4096, 2, 7168], P(('dp', 'expert'), None, 'tile'), may hold values from -6 to 6
- routes: int32 [4096, 2], P(('dp', 'expert')), may hold values from 0 to 7, all different within a row; in each aligned block of 64 rows (0 to 63, 64 to 127, ...) at most 24 rows name the same one
- lengths: int32 [64], P(('dp', 'expert')), may hold values from 1 to 64, as said below
Outputs:
- hessian_in: float32 [8, 4096, 4096], P('expert', 'tile', 'dp')
- hessian_down: float32 [8, 7168, 7168], P('expert', 'tile', 'dp')
The draws below stay inside these ranges and needn't reach their ends.
Inputs may be any that keep to these rules, and one draw needn't show every extreme that they name: `routes`: in each aligned block of 64 rows (the rows of one group) no expert is named by more than 24 rows, a bound that some block reaches. The live rows of group g are its first lengths[g] rows; the last group is full.
All inputs are finite; a program needn't handle non-finite values.
Results may differ from the reference program's by a relative error of at most 0.0003.
Values may be sent and summed in bfloat16 or wider, within the bound.
A program may use at most 64 MiB of HBM per device.

```python
import math
import jax
import jax.numpy as jnp
import numpy as np
from jax import lax

D = 4096
FFW = 7168
TOP = 2
TOK_DEV = 64
EXPERTS = 8
GROUPS = 64
TOKENS = 4096
CAP = 24


def draw_lengths(key, part):
    group_index = jnp.arange(GROUPS, dtype=jnp.int32)
    lowest = TOK_DEV // 3
    rising = lowest + (TOK_DEV - lowest) * group_index // max(GROUPS - 1, 1)
    jitter = jax.random.randint(key, (GROUPS,), 0, max(TOK_DEV // 8, 1), dtype=jnp.int32)
    jitter = jnp.where(group_index == GROUPS - 1, 0, jitter)
    return jnp.maximum(rising - jitter, 1).astype(jnp.int32)


def steps_of(stream_key, dims, shards, low, top_value):
    gain = 1.0
    for axis_at, parts in shards:
        heights = jax.random.uniform(jax.random.fold_in(jax.random.fold_in(stream_key, 6), axis_at), (parts,), jnp.float32, low / len(shards), top_value / len(shards))
        gain = gain * jnp.repeat(jnp.exp(heights), dims[axis_at] // parts).reshape((-1,) + (1,) * (len(dims) - 1 - axis_at))
    return gain


def assign_block(own_key, own, number, rows, number_of, top, bound, slope):
    order = jax.random.permutation(own_key, number_of)
    crowded, ordinary = portions_of(number_of, rows * top, bound, slope, True), portions_of(number_of, rows * top, bound, slope, False)
    places = jnp.arange(number_of)

    def named(sizes, rotation):
        used = int((sizes > 0).sum())
        fixed = max(1, used // 4)
        passed = fixed + (places - fixed + rotation * (used - fixed)) % max(1, number_of - fixed)
        return jnp.zeros((number_of,), jnp.int32).at[order[jnp.where(places < fixed, places, passed)]].set(jnp.asarray(sizes, jnp.int32))

    sizes = jnp.where(number % 4 == 0, named(crowded, number // 4), named(ordinary, number - number // 4 - 1))
    mixed = jax.random.permutation(jax.random.fold_in(own, 3), number_of)
    source_of, receiver = mixed[0:number_of // 2 * 2:2], mixed[1:number_of // 2 * 2:2]
    room = jnp.minimum(sizes[source_of] - 1, bound - sizes[receiver]) // 2
    room = jnp.where((source_of == order[0]) | (receiver == order[0]) | (sizes[receiver] == 0), 0, jnp.maximum(room, 0))
    passed = jax.random.randint(jax.random.fold_in(own, 4), (number_of // 2,), 0, 1 << 20) % (room + 1)
    sizes = sizes.at[source_of].add(-passed).at[receiver].add(passed)
    members = jnp.searchsorted(jnp.cumsum(sizes), jnp.arange(rows * top), side="right").astype(jnp.int32)
    grid = members.reshape(top, rows).T
    grid = grid[jax.random.permutation(jax.random.fold_in(own, 1), rows)]
    rotation = jax.random.randint(jax.random.fold_in(own, 2), (rows, 1), 0, top)
    return jnp.take_along_axis(grid, (jnp.arange(top)[None, :] + rotation) % top, axis=1)


def portions_of(count, total, limit, slope, full):
    loads = [(1 << 20) // math.isqrt(rank ** slope) + 1 for rank in range(1, count + 1)]
    largest = limit if full else min(limit, max(-(-total // count), total * loads[0] // sum(loads)))
    least = 1 if total - largest >= count - 1 else 0
    counts, spare = [largest] + [least] * (count - 1), total - largest - least * (count - 1)
    while spare > 0:
        candidates = [i for i in range(1, count) if counts[i] < largest] or [i for i in range(1, count) if counts[i] < limit]
        pool, budget = sum([loads[i] for i in candidates]), spare
        for i in candidates:
            addition = min(limit - counts[i], max(1, budget * loads[i] // pool), spare)
            counts[i] = counts[i] + addition
            spare = spare - addition
    return np.array(counts)


def gaussian(key, shape, spread, reach, pieces=(), kind=jnp.bfloat16):
    drawn = jax.random.normal(key, shape, jnp.float32) * spread
    if len(pieces) > 0:
        drawn = steps_of(key, shape, pieces, -0.22, 0.18) * drawn
    return jnp.clip(drawn, min=-reach, max=reach).astype(kind)


def setup_inputs(seed: int = 0) -> dict:
    streams_of = jax.random.split(jax.random.key(seed), 5)
    tokens = gaussian(streams_of[0], (TOKENS, D), 1.0, 6.0, ((0, 64), (1, 4)))
    hidden = gaussian(streams_of[1], (TOKENS, TOP, FFW), 1.0, 6.0, ((0, 64), (2, 4)))
    routes_keys = jax.random.split(jax.random.fold_in(streams_of[2], 1), TOKENS // TOK_DEV)
    routes_turns = jax.random.permutation(jax.random.fold_in(streams_of[2], 3), TOKENS // TOK_DEV)
    routes = jax.vmap(lambda own, number: assign_block(jax.random.fold_in(streams_of[2], 2), own, number, TOK_DEV, EXPERTS, TOP, CAP, 1))(routes_keys, routes_turns).reshape((TOKENS, TOP))
    lengths = draw_lengths(jax.random.fold_in(streams_of[4], 71), 0)
    return dict(tokens=tokens, hidden=hidden, routes=routes, lengths=lengths)


def reference(tokens, hidden, routes, lengths):
    token_total = tokens.shape[0]
    token_index = jnp.arange(token_total, dtype=jnp.int32)
    live_mask = (token_index % TOK_DEV) < lengths[token_index // TOK_DEV]
    row_limit = GROUPS * CAP

    def one_expert(expert):
        picked = (routes == expert) & live_mask[:, None]
        token_hit = jnp.any(picked, axis=1)
        pair_count = jnp.sum(picked.astype(jnp.float32))
        ordering = jnp.argsort(jnp.where(token_hit, 0, 1).astype(jnp.int32), stable=True)[:row_limit]
        chosen = tokens[ordering] * token_hit[ordering][:, None].astype(jnp.bfloat16)
        weights = picked[ordering].astype(jnp.float32)
        chosen_hidden = jnp.sum(hidden[ordering].astype(jnp.float32) * weights[:, :, None], axis=1).astype(jnp.bfloat16)
        factor = jnp.float32(2.0) / jnp.maximum(pair_count, jnp.float32(1.0))
        gram_tokens = jnp.dot(chosen.T, chosen, preferred_element_type=jnp.float32) * factor
        gram_hidden = jnp.dot(chosen_hidden.T, chosen_hidden, preferred_element_type=jnp.float32) * factor
        return gram_tokens, gram_hidden

    hessian_in, hessian_down = lax.map(one_expert, jnp.arange(EXPERTS, dtype=jnp.int32))
    return hessian_in, hessian_down
```

```python
import functools

import jax
import jax.numpy as jnp
from jax import lax
from jax.experimental import pallas as pl
from jax.experimental.pallas import tpu as pltpu
from jax.sharding import PartitionSpec as P

MESH = pl.DeviceIdType.MESH
CAP = 24
ROWS = 2 * CAP


def positions(eff, experts, base):
    pairs = eff.shape[1]
    expert = lax.broadcasted_iota(jnp.int32, (experts, pairs), 0)
    hit = jnp.where(eff == expert, 1.0, 0.0)
    earlier = lax.broadcasted_iota(jnp.int32, (pairs, pairs), 0) < lax.broadcasted_iota(
        jnp.int32, (pairs, pairs), 1
    )
    before = jnp.dot(
        hit.astype(jnp.bfloat16),
        jnp.where(earlier, 1.0, 0.0).astype(jnp.bfloat16),
        preferred_element_type=jnp.float32,
    )
    rank = jnp.sum(hit * before, axis=0, keepdims=True).astype(jnp.int32)
    return eff * ROWS + base + rank


def exchange_kernel(
    nz, ny, nx,
    eff_ref, hid_ref, tok_ref,
    xh_out, xt_out, yh_out, yt_out, factor_out,
    eff_p, hid_p, tok_p, gath, xb, xo, yb, cs, cr, ys, yr,
    pair_s, pair_r, zs, zr, ysend, yrecv, xsend, xrecv, ds, dr, cz_s, cz_r, cy_s, cy_r, local_sem,
):
    d, z, x = lax.axis_index("dp"), lax.axis_index("expert"), lax.axis_index("tile")
    y, c = d // 2, d % 2
    wh = hid_ref.shape[1] // 2
    wt = tok_ref.shape[1] // 2

    def device(yy, cc, zz, xx):
        return {"dp": yy * 2 + cc, "expert": zz, "tile": xx}

    step = 1 - 2 * c
    y_next = lax.rem(y + step + ny, ny)
    x_next = lax.rem(x + step + nx, nx)
    place = lax.rem((x - y) * step + 2 * nx, nx)
    partner = device(y, 1 - c, z, x)
    to_y, to_x = device(y_next, c, z, x), device(y, c, z, x_next)

    def z_offset(k):
        return lax.rem(jnp.where(k % 2 == 1, (k + 1) // 2, nz - k // 2), nz)

    barrier = pltpu.get_barrier_semaphore()
    for o in range(1, nz):
        pl.semaphore_signal(barrier, inc=1, device_id=device(y, c, lax.rem(z + o, nz), x), device_id_type=MESH)
    for o in range(1, ny):
        pl.semaphore_signal(barrier, inc=1, device_id=device(lax.rem(y + o, ny), c, z, x), device_id_type=MESH)
    for o in (1, nx - 1):
        pl.semaphore_signal(barrier, inc=1, device_id=device(y, c, z, lax.rem(x + o, nx)), device_id_type=MESH)
    pl.semaphore_signal(barrier, inc=1, device_id=partner, device_id_type=MESH)
    pl.semaphore_wait(barrier, nz - 1 + ny - 1 + 2 + 1)

    def remote(src, dst, s, r, to):
        return pltpu.make_async_remote_copy(
            src_ref=src, dst_ref=dst, send_sem=s, recv_sem=r, device_id=to, device_id_type=MESH
        )

    theirs_h = pl.ds(pl.multiple_of((1 - c) * wh, 128), wh)
    theirs_t = pl.ds(pl.multiple_of((1 - c) * wt, 128), wt)
    swaps = (
        remote(eff_ref, eff_p, pair_s.at[0], pair_r.at[0], partner),
        remote(hid_ref.at[:, theirs_h], hid_p, pair_s.at[1], pair_r.at[1], partner),
        remote(tok_ref.at[:, theirs_t], tok_p, pair_s.at[2], pair_r.at[2], partner),
    )
    for s in swaps:
        s.start()
    eff_mine = eff_ref[...]
    mine_h = hid_ref[:, pl.ds(pl.multiple_of(c * wh, 128), wh)]
    mine_t = tok_ref[:, pl.ds(pl.multiple_of(c * wt, 128), wt)]
    mine_t2 = jnp.concatenate([mine_t, mine_t], axis=0)
    slot_mine = positions(eff_mine, nz, c * CAP)
    for s in swaps:
        s.wait_recv()
    eff_theirs = eff_p[...]
    slot_theirs = positions(eff_theirs, nz, (1 - c) * CAP)
    pairs = eff_mine.shape[1]

    def gathered(e, out):
        slot = lax.broadcasted_iota(jnp.int32, (ROWS, pairs), 0) + e * ROWS
        a = jnp.where(slot == slot_mine, 1.0, 0.0).astype(jnp.bfloat16)
        b = jnp.where(slot == slot_theirs, 1.0, 0.0).astype(jnp.bfloat16)
        their_t = tok_p[...]
        out[:, :wh] = (
            jnp.dot(a, mine_h, preferred_element_type=jnp.float32)
            + jnp.dot(b, hid_p[...], preferred_element_type=jnp.float32)
        ).astype(jnp.bfloat16)
        out[:, wh:] = (
            jnp.dot(a, mine_t2, preferred_element_type=jnp.float32)
            + jnp.dot(b, jnp.concatenate([their_t, their_t], axis=0), preferred_element_type=jnp.float32)
        ).astype(jnp.bfloat16)

    def tally(e):
        hits = jnp.where(eff_mine == e, 1.0, 0.0) + jnp.where(eff_theirs == e, 1.0, 0.0)
        return jnp.broadcast_to(jnp.sum(hits, axis=1, keepdims=True), (8, 128))

    gathered(z, xb.at[0, y])

    def z_copy(k):
        to = device(y, c, lax.rem(z + nz - z_offset(k), nz), x)
        return remote(gath.at[k], xb.at[k, y], zs.at[k], zr.at[k], to)

    def count_copy(k):
        to = device(y, c, lax.rem(z + nz - z_offset(k), nz), x)
        return remote(cs.at[k], cr.at[k], cz_s.at[k], cz_r.at[k], to)

    def fill(k, carry):
        e = lax.rem(z + nz - z_offset(k), nz)
        gathered(e, gath.at[k])
        cs[k] = tally(e)
        z_copy(k).start()
        count_copy(k).start()
        return carry

    lax.fori_loop(1, nz, fill, 0)

    def row_of(h):
        return lax.rem(y + ny * h - h * step, ny)

    def y_copy(k, h):
        yy = row_of(h)
        return remote(xb.at[k, yy], xb.at[k, yy], ysend.at[k, h], yrecv.at[k, h + 1], to_y)

    def y_arrival(k, h):
        yy = row_of(h)
        return remote(xb.at[k, yy], xb.at[k, yy], ysend.at[k, h - 1], yrecv.at[k, h], to_y)

    def x_first(k, h):
        yy = row_of(h)
        return remote(xb.at[k, yy], yb.at[k, yy], xsend.at[k, h], xrecv.at[k, h], to_x)

    def x_copy(k, h):
        yy = row_of(h)
        return remote(yb.at[k, yy], yb.at[k, yy], xsend.at[k, h], xrecv.at[k, h], to_x)

    def d_copy(k):
        return remote(xb.at[k], xo.at[k], ds.at[k], dr.at[k], partner)

    def outs_of(k, src, half, at):
        return (
            pltpu.make_async_copy(src.at[k, :, :, pl.ds(0, wh)], xh_out.at[half, k], local_sem.at[k, at]),
            pltpu.make_async_copy(src.at[k, :, :, pl.ds(wh, wt)], xt_out.at[half, k], local_sem.at[k, at + 1]),
        )

    def outs_y(k, src):
        return (
            pltpu.make_async_copy(src.at[k, :, :, pl.ds(0, wh)], yh_out.at[k], local_sem.at[k, 4]),
            pltpu.make_async_copy(src.at[k, :, :, pl.ds(wh, wt)], yt_out.at[k], local_sem.at[k, 5]),
        )

    def starts(copies):
        for copy in copies:
            copy.start()

    lag = place + 1

    def round_of(i, carry):
        @pl.when(i < nz)
        def _():
            @pl.when(i > 0)
            def _():
                z_copy(i).wait_recv()

            y_copy(i, 0).start()

            @pl.when(place == 0)
            def _():
                x_first(i, 0).start()

        for h in range(1, ny):
            k = i - h

            @pl.when((k >= 0) & (k < nz))
            def _():
                y_arrival(k, h).wait_recv()
                if h < ny - 1:
                    y_copy(k, h).start()

                @pl.when(place == 0)
                def _():
                    x_first(k, h).start()

                if h == ny - 1:
                    d_copy(k).start()
                    starts(outs_of(k, xb, c, 0))

                    @pl.when(place == 0)
                    def _():
                        starts(outs_y(k, xb))

        @pl.when(place > 0)
        def _():
            for h in range(ny):
                k = i - lag - h

                @pl.when((k >= 0) & (k < nz))
                def _():
                    x_first(k, h).wait_recv()

                    @pl.when(place < nx - 1)
                    def _():
                        x_copy(k, h).start()

                    if h == ny - 1:
                        starts(outs_y(k, yb))

        k_out = i - ny - 1

        @pl.when((k_out >= 0) & (k_out < nz))
        def _():
            d_copy(k_out).wait_recv()
            starts(outs_of(k_out, xo, 1 - c, 2))

        return carry

    lax.fori_loop(0, nz, round_of, 0)

    total = tally(z)
    for k in range(1, nz):
        count_copy(k).wait_recv()
        total = total + cr[k]
    ys[...] = total

    def tally_copy(h):
        return remote(ys, yr.at[h], cy_s.at[h], cy_r.at[h], device(lax.rem(y + h, ny), c, z, x))

    for h in range(1, ny):
        tally_copy(h).start()

    lax.fori_loop(nz, nz + ny + nx - 1, round_of, 0)

    for h in range(1, ny):
        tally_copy(h).wait_recv()
        total = total + yr[h]
    factor_out[...] = 2.0 / jnp.maximum(total, 1.0)

    for s in swaps:
        s.wait_send()
    for h in range(1, ny):
        tally_copy(h).wait_send()

    def finish(k, carry):
        @pl.when(k > 0)
        def _():
            z_copy(k).wait_send()
            count_copy(k).wait_send()

        for h in range(ny - 1):
            y_copy(k, h).wait_send()
        for h in range(ny):

            @pl.when(place < nx - 1)
            def _():
                x_copy(k, h).wait_send()

        d_copy(k).wait_send()
        for copy in outs_of(k, xb, c, 0) + outs_of(k, xo, 1 - c, 2) + outs_y(k, yb):
            copy.wait()
        return carry

    lax.fori_loop(0, nz, finish, 0)


def exchange(eff, hid, tok, nz, ny, nx):
    wh, wt = hid.shape[1] // 2, tok.shape[1] // 2
    pairs, tokens = hid.shape[0], tok.shape[0]
    bf, f32 = jnp.bfloat16, jnp.float32
    any_spec = pl.BlockSpec(memory_space=pl.ANY)
    vmem = pl.BlockSpec(memory_space=pltpu.VMEM)
    dma = pltpu.SemaphoreType.DMA
    piece = (nz, ny, ROWS, wh + wt)
    return pl.pallas_call(
        functools.partial(exchange_kernel, nz, ny, nx),
        out_shape=(
            jax.ShapeDtypeStruct((2, nz, ny, ROWS, wh), bf),
            jax.ShapeDtypeStruct((2, nz, ny, ROWS, wt), bf),
            jax.ShapeDtypeStruct((nz, ny, ROWS, wh), bf),
            jax.ShapeDtypeStruct((nz, ny, ROWS, wt), bf),
            jax.ShapeDtypeStruct((8, 128), f32),
        ),
        in_specs=[vmem] * 3,
        out_specs=(any_spec,) * 4 + (vmem,),
        scratch_shapes=[
            pltpu.VMEM((1, pairs), jnp.int32),
            pltpu.VMEM((pairs, wh), bf),
            pltpu.VMEM((tokens, wt), bf),
            pltpu.VMEM((nz, ROWS, wh + wt), bf),
            pltpu.VMEM(piece, bf),
            pltpu.VMEM(piece, bf),
            pltpu.VMEM(piece, bf),
            pltpu.VMEM((nz, 8, 128), f32),
            pltpu.VMEM((nz, 8, 128), f32),
            pltpu.VMEM((8, 128), f32),
            pltpu.VMEM((ny, 8, 128), f32),
            dma((3,)), dma((3,)),
            dma((nz,)), dma((nz,)),
            dma((nz, ny)), dma((nz, ny)),
            dma((nz, ny)), dma((nz, ny)),
            dma((nz,)), dma((nz,)),
            dma((nz,)), dma((nz,)),
            dma((ny,)), dma((ny,)),
            dma((nz, 6)),
        ],
        compiler_params=pltpu.CompilerParams(
            collective_id=0, has_side_effects=True, vmem_limit_bytes=40 * 1024 * 1024
        ),
        cost_estimate=pl.CostEstimate(flops=10**9, bytes_accessed=20 * 2**20, transcendentals=0),
    )(eff, hid, tok)


def on_device(tokens, hidden, routes, lengths):
    nz = lax.axis_size("expert")
    ny = lax.axis_size("dp") // 2
    nx = lax.axis_size("tile")
    token_count, top, width = hidden.shape
    live = jnp.arange(token_count, dtype=jnp.int32) < lengths[0]
    eff = jnp.where(live[None, :], routes.T, nz).reshape(1, top * token_count)
    hid = hidden.transpose(1, 0, 2).reshape(top * token_count, width)
    xh, xt, yh, yt, factor = exchange(eff, hid, tokens, nz, ny, nx)
    rows = nz * ny * ROWS

    def gram(left, right):
        left = left.reshape(2, rows, left.shape[-1])
        right = right.reshape(rows, right.shape[-1])
        out = lax.dot_general(left, right, (((1,), (0,)), ((), ())), preferred_element_type=jnp.float32)
        return (out * factor[0, 0]).reshape(1, 2 * left.shape[-1], right.shape[-1])

    return gram(xt, yt), gram(xh, yh)


def solution(mesh):
    placed = (
        P(("dp", "expert"), "tile"),
        P(("dp", "expert"), None, "tile"),
        P(("dp", "expert"), None),
        P(("dp", "expert")),
    )
    return jax.shard_map(
        on_device,
        mesh=mesh,
        in_specs=placed,
        out_specs=(P("expert", "tile", "dp"), P("expert", "tile", "dp")),
        check_vma=False,
    )
```

```python
import functools

import jax
import jax.numpy as jnp
from jax import lax
from jax.experimental import pallas as pl
from jax.experimental.pallas import tpu as pltpu
from jax.sharding import PartitionSpec as P

MESH = pl.DeviceIdType.MESH
CAP = 24
ROWS = 2 * CAP
LAST = 1


def positions(eff, experts, base):
    pairs = eff.shape[1]
    expert = lax.broadcasted_iota(jnp.int32, (experts, pairs), 0)
    hit = jnp.where(eff == expert, 1.0, 0.0)
    earlier = lax.broadcasted_iota(jnp.int32, (pairs, pairs), 0) < lax.broadcasted_iota(
        jnp.int32, (pairs, pairs), 1
    )
    before = jnp.dot(
        hit.astype(jnp.bfloat16),
        jnp.where(earlier, 1.0, 0.0).astype(jnp.bfloat16),
        preferred_element_type=jnp.float32,
    )
    rank = jnp.sum(hit * before, axis=0, keepdims=True).astype(jnp.int32)
    return eff * ROWS + base + rank


def exchange_kernel(
    nz, ny, nx,
    eff_ref, hid_ref, tok_ref,
    xs, yb, acc_h, acc_t, factor_out,
    eff_p, hid_p, tok_p, gath, cs, cr, ys, yr,
    pair_s, pair_r, zs, zr, ysend, yrecv, xsend, xrecv, ds, dr, cz_s, cz_r, cy_s, cy_r, local_sem,
):
    d, z, x = lax.axis_index("dp"), lax.axis_index("expert"), lax.axis_index("tile")
    y, c = d // 2, d % 2
    wh = hid_ref.shape[1] // 2
    wt = tok_ref.shape[1] // 2

    def device(yy, cc, zz, xx):
        return {"dp": yy * 2 + cc, "expert": zz, "tile": xx}

    step = 1 - 2 * c
    y_next = lax.rem(y + step + ny, ny)
    x_next = lax.rem(x + step + nx, nx)
    place = lax.rem((x - y) * step + 2 * nx, nx)
    partner = device(y, 1 - c, z, x)
    to_y, to_x = device(y_next, c, z, x), device(y, c, z, x_next)

    def z_offset(k):
        return lax.rem(jnp.where(k % 2 == 1, (k + 1) // 2, nz - k // 2), nz)

    barrier = pltpu.get_barrier_semaphore()
    for o in range(1, nz):
        pl.semaphore_signal(barrier, inc=1, device_id=device(y, c, lax.rem(z + o, nz), x), device_id_type=MESH)
    for o in range(1, ny):
        pl.semaphore_signal(barrier, inc=1, device_id=device(lax.rem(y + o, ny), c, z, x), device_id_type=MESH)
    for o in (1, nx - 1):
        pl.semaphore_signal(barrier, inc=1, device_id=device(y, c, z, lax.rem(x + o, nx)), device_id_type=MESH)
    pl.semaphore_signal(barrier, inc=1, device_id=partner, device_id_type=MESH)

    def remote(src, dst, s, r, to):
        return pltpu.make_async_remote_copy(
            src_ref=src, dst_ref=dst, send_sem=s, recv_sem=r, device_id=to, device_id_type=MESH
        )

    theirs_h = pl.ds(pl.multiple_of((1 - c) * wh, 128), wh)
    theirs_t = pl.ds(pl.multiple_of((1 - c) * wt, 128), wt)
    swaps = (
        remote(eff_ref, eff_p, pair_s.at[0], pair_r.at[0], partner),
        remote(hid_ref.at[:, theirs_h], hid_p, pair_s.at[1], pair_r.at[1], partner),
        remote(tok_ref.at[:, theirs_t], tok_p, pair_s.at[2], pair_r.at[2], partner),
    )
    pl.semaphore_wait(barrier, nz - 1 + ny - 1 + 2 + 1)
    for s in swaps:
        s.start()
    eff_mine = eff_ref[...]
    mine_h = hid_ref[:, pl.ds(pl.multiple_of(c * wh, 128), wh)]
    mine_t = tok_ref[:, pl.ds(pl.multiple_of(c * wt, 128), wt)]
    mine_t2 = jnp.concatenate([mine_t, mine_t], axis=0)
    slot_mine = positions(eff_mine, nz, c * CAP)
    for s in swaps:
        s.wait_recv()
    eff_theirs = eff_p[...]
    slot_theirs = positions(eff_theirs, nz, (1 - c) * CAP)
    pairs = eff_mine.shape[1]

    def gathered(e, out):
        slot = lax.broadcasted_iota(jnp.int32, (ROWS, pairs), 0) + e * ROWS
        a = jnp.where(slot == slot_mine, 1.0, 0.0).astype(jnp.bfloat16)
        b = jnp.where(slot == slot_theirs, 1.0, 0.0).astype(jnp.bfloat16)
        their_t = tok_p[...]
        out[:, :wh] = (
            jnp.dot(a, mine_h, preferred_element_type=jnp.float32)
            + jnp.dot(b, hid_p[...], preferred_element_type=jnp.float32)
        ).astype(jnp.bfloat16)
        out[:, wh:] = (
            jnp.dot(a, mine_t2, preferred_element_type=jnp.float32)
            + jnp.dot(b, jnp.concatenate([their_t, their_t], axis=0), preferred_element_type=jnp.float32)
        ).astype(jnp.bfloat16)

    def tally(e):
        hits = jnp.where(eff_mine == e, 1.0, 0.0) + jnp.where(eff_theirs == e, 1.0, 0.0)
        return jnp.broadcast_to(jnp.sum(hits, axis=1, keepdims=True), (8, 128))

    def z_copy(k):
        to = device(y, c, lax.rem(z + nz - z_offset(k), nz), x)
        return remote(gath.at[k], xs.at[c, k, y], zs.at[k], zr.at[k], to)

    def count_copy(k):
        to = device(y, c, lax.rem(z + nz - z_offset(k), nz), x)
        return remote(cs.at[k], cr.at[k], cz_s.at[k], cz_r.at[k], to)

    def row_of(h):
        return lax.rem(y + ny * h - h * step, ny)

    def y_copy(k, h):
        here = xs.at[c, k, row_of(h)]
        return remote(here, here, ysend.at[k, h], yrecv.at[k, h + 1], to_y)

    def y_arrival(k, h):
        here = xs.at[c, k, row_of(h)]
        return remote(here, here, ysend.at[k, h - 1], yrecv.at[k, h], to_y)

    def x_first(k, h):
        yy = row_of(h)
        return remote(xs.at[c, k, yy], yb.at[k, yy], xsend.at[k, h], xrecv.at[k, h], to_x)

    def x_copy(k, h):
        here = yb.at[k, row_of(h)]
        return remote(here, here, xsend.at[k, h], xrecv.at[k, h], to_x)

    def d_copy(k):
        return remote(xs.at[c, k], xs.at[c, k], ds.at[k], dr.at[k], partner)

    def d_arrival(k):
        return remote(xs.at[1 - c, k], xs.at[1 - c, k], ds.at[k], dr.at[k], partner)

    def columns_copy(k):
        return pltpu.make_async_copy(xs.at[c, k], yb.at[k], local_sem.at[k])

    def first_step(k):
        y_copy(k, 0).start()

        @pl.when(place == 0)
        def _():
            x_first(k, 0).start()

    gathered(z, xs.at[c, 0, y])
    first_step(0)

    def fill(k, carry):
        e = lax.rem(z + nz - z_offset(k), nz)
        gathered(e, gath.at[k])
        z_copy(k).start()
        cs[k] = tally(e)
        count_copy(k).start()
        return carry

    lax.fori_loop(1, nz, fill, 0)

    def add_product(k, half, lo, size, acc, first, width, row):
        left = xs[half, k, :, :, lo : lo + size].reshape(ny * ROWS, size)
        right = yb[k, :, :, first : first + width].reshape(ny * ROWS, width)
        part = lax.dot_general(left, right, (((0,), (0,)), ((), ())), preferred_element_type=jnp.float32)
        rows = pl.ds(row, size)

        @pl.when(k == 0)
        def _():
            acc[rows, :] = part

        @pl.when(k > 0)
        def _():
            acc[rows, :] += part

    def product(k, half, part):
        tiles = hidden_tiles(wh)
        if part < len(tiles):
            lo, size = tiles[part]
            add_product(k, half, lo, size, acc_h, 0, wh, half * wh + lo)
        else:
            add_product(k, half, wh, wt, acc_t, wh, wt, half * wt)

    parts = len(hidden_tiles(wh)) + 1

    def round_of(i, carry):
        k_dot = i - ny - place
        dot_now = (k_dot >= 0) & (k_dot < nz - LAST)

        @pl.when(i < nz)
        def _():
            z_copy(i).wait_recv()
            first_step(i)

        for h in range(1, ny):
            k = i - h

            @pl.when((k >= 0) & (k < nz))
            def _():
                y_arrival(k, h).wait_recv()
                if h < ny - 1:
                    y_copy(k, h).start()

                @pl.when(place == 0)
                def _():
                    x_first(k, h).start()

                if h == ny - 1:
                    d_copy(k).start()

                    @pl.when(place == 0)
                    def _():
                        columns_copy(k).start()

            if h == 1:

                @pl.when(dot_now)
                def _():
                    d_arrival(k_dot).wait_recv()

                    @pl.when(place == 0)
                    def _():
                        columns_copy(k_dot).wait()

                    for part in range(parts):
                        product(k_dot, 0, part)

        @pl.when(i == nz - 1)
        def _():
            total = tally(z)
            for k in range(1, nz):
                count_copy(k).wait_recv()
                total = total + cr[k]
            ys[...] = total
            for h in range(1, ny):
                tally_copy(h).start()

        for h in range(ny):
            k = i - place - h

            @pl.when((place > 0) & (k >= 0) & (k < nz))
            def _():
                x_first(k, h).wait_recv()

                @pl.when(place < nx - 1)
                def _():
                    x_copy(k, h).start()

            if h == 1:

                @pl.when(dot_now)
                def _():
                    for part in range(parts):
                        product(k_dot, 1, part)

        return carry

    def tally_copy(h):
        return remote(ys, yr.at[h], cy_s.at[h], cy_r.at[h], device(lax.rem(y + h, ny), c, z, x))

    lax.fori_loop(1, nz + ny + nx - 2, round_of, 0)

    total = ys[...]
    for h in range(1, ny):
        tally_copy(h).wait_recv()
        total = total + yr[h]
    factor_out[...] = 2.0 / jnp.maximum(total, 1.0)

    for k in range(nz - LAST, nz):
        d_arrival(k).wait_recv()

        @pl.when(place == 0)
        def _():
            columns_copy(k).wait()

    for s in swaps:
        s.wait_send()
    for h in range(1, ny):
        tally_copy(h).wait_send()

    def finish(k, carry):
        @pl.when(k > 0)
        def _():
            z_copy(k).wait_send()
            count_copy(k).wait_send()

        for h in range(ny - 1):
            y_copy(k, h).wait_send()
        for h in range(ny):

            @pl.when(place < nx - 1)
            def _():
                x_copy(k, h).wait_send()

        d_copy(k).wait_send()
        return carry

    lax.fori_loop(0, nz, finish, 0)


def hidden_tiles(width):
    half = width // 256 * 128
    return ((0, half), (half, width - half)) if half else ((0, width),)


def exchange(eff, hid, tok, nz, ny, nx):
    wh, wt = hid.shape[1] // 2, tok.shape[1] // 2
    pairs, tokens = hid.shape[0], tok.shape[0]
    bf, f32 = jnp.bfloat16, jnp.float32
    vmem = pl.BlockSpec(memory_space=pltpu.VMEM)
    dma = pltpu.SemaphoreType.DMA
    piece = (nz, ny, ROWS, wh + wt)
    return pl.pallas_call(
        functools.partial(exchange_kernel, nz, ny, nx),
        out_shape=(
            jax.ShapeDtypeStruct((2, *piece), bf),
            jax.ShapeDtypeStruct(piece, bf),
            jax.ShapeDtypeStruct((2 * wh, wh), f32),
            jax.ShapeDtypeStruct((2 * wt, wt), f32),
            jax.ShapeDtypeStruct((8, 128), f32),
        ),
        in_specs=[vmem] * 3,
        out_specs=(vmem,) * 5,
        scratch_shapes=[
            pltpu.VMEM((1, pairs), jnp.int32),
            pltpu.VMEM((pairs, wh), bf),
            pltpu.VMEM((tokens, wt), bf),
            pltpu.VMEM((nz, ROWS, wh + wt), bf),
            pltpu.VMEM((nz, 8, 128), f32),
            pltpu.VMEM((nz, 8, 128), f32),
            pltpu.VMEM((8, 128), f32),
            pltpu.VMEM((ny, 8, 128), f32),
            dma((3,)), dma((3,)),
            dma((nz,)), dma((nz,)),
            dma((nz, ny)), dma((nz, ny)),
            dma((nz, ny)), dma((nz, ny)),
            dma((nz,)), dma((nz,)),
            dma((nz,)), dma((nz,)),
            dma((ny,)), dma((ny,)),
            dma((nz,)),
        ],
        compiler_params=pltpu.CompilerParams(
            collective_id=0, has_side_effects=True, vmem_limit_bytes=12 * 1024 * 1024
        ),
        cost_estimate=pl.CostEstimate(flops=6 * 10**9, bytes_accessed=20 * 2**20, transcendentals=0),
    )(eff, hid, tok)


def finish_kernel(nz, xs, yb, acc_h, acc_t, factor_ref, out_h, out_t, res_h, res_t, sem):
    ny = xs.shape[2]
    wh, wt = acc_h.shape[1], acc_t.shape[1]
    depth = LAST * ny * ROWS
    factor = factor_ref[0:1, 0:1]
    copies = []
    for half in range(2):
        tiles = [(lo, size, half * wh + lo, acc_h, res_h, out_h, 0, wh) for lo, size in hidden_tiles(wh)]
        tiles.append((wh, wt, half * wt, acc_t, res_t, out_t, wh, wh + wt))
        for lo, size, row, acc, res, out, first, last in tiles:
            left = xs[half, nz - LAST :, :, :, lo : lo + size].reshape(depth, size)
            right = yb[nz - LAST :, :, :, first:last].reshape(depth, last - first)
            part = lax.dot_general(left, right, (((0,), (0,)), ((), ())), preferred_element_type=jnp.float32)
            res[row : row + size, :] = (acc[row : row + size, :] + part) * factor
            copy = pltpu.make_async_copy(
                res.at[pl.ds(row, size), :], out.at[0, pl.ds(row, size), :], sem.at[len(copies)]
            )
            copy.start()
            copies.append(copy)
    for copy in copies:
        copy.wait()


def finish(xs, yb, acc_h, acc_t, factor, nz):
    f32 = jnp.float32
    any_spec = pl.BlockSpec(memory_space=pl.ANY)
    vmem = pl.BlockSpec(memory_space=pltpu.VMEM)
    return pl.pallas_call(
        functools.partial(finish_kernel, nz),
        out_shape=(
            jax.ShapeDtypeStruct((1, *acc_h.shape), f32),
            jax.ShapeDtypeStruct((1, *acc_t.shape), f32),
        ),
        in_specs=[vmem] * 5,
        out_specs=(any_spec, any_spec),
        scratch_shapes=[
            pltpu.VMEM(acc_h.shape, f32),
            pltpu.VMEM(acc_t.shape, f32),
            pltpu.SemaphoreType.DMA((2 * len(hidden_tiles(acc_h.shape[1])) + 2,)),
        ],
        compiler_params=pltpu.CompilerParams(vmem_limit_bytes=12 * 1024 * 1024),
        cost_estimate=pl.CostEstimate(flops=10**9, bytes_accessed=9 * 2**20, transcendentals=0),
    )(xs, yb, acc_h, acc_t, factor)


def on_device(tokens, hidden, routes, lengths):
    nz = lax.axis_size("expert")
    ny = lax.axis_size("dp") // 2
    nx = lax.axis_size("tile")
    token_count, top, width = hidden.shape
    live = jnp.arange(token_count, dtype=jnp.int32) < lengths[0]
    eff = jnp.where(live[None, :], routes.T, nz).reshape(1, top * token_count)
    hid = hidden.transpose(1, 0, 2).reshape(top * token_count, width)
    xs, yb, acc_h, acc_t, factor = exchange(eff, hid, tokens, nz, ny, nx)
    down, into = finish(xs, yb, acc_h, acc_t, factor, nz)
    return into, down


def solution(mesh):
    placed = (
        P(("dp", "expert"), "tile"),
        P(("dp", "expert"), None, "tile"),
        P(("dp", "expert"), None),
        P(("dp", "expert")),
    )
    return jax.shard_map(
        on_device,
        mesh=mesh,
        in_specs=placed,
        out_specs=(P("expert", "tile", "dp"), P("expert", "tile", "dp")),
        check_vma=False,
    )
```
